512 devices in a mesh: layer: 8 (over y, z_hi), row: 4 (over x), col: 16 (over z_lo, core).
Axes of the slice: x: 4, y: 4, z: 16 (z_hi: 2, z_lo: 8; z = z_hi * 8 + z_lo), core: 2. Of those that a mesh axis runs over, the one named last changes fastest.
Arguments:
- subtree_terms: float32 [8, 4096, 4096], P('layer', 'row', 'col')
- order: int32 [2], replicated, may hold values from 0 to 1, each once
Outputs:
- factored: float32 [4096, 4096], P('row', 'col')
The draws below stay inside these ranges and needn't reach their ends.
Inputs may be any that keep to these rules, and one draw needn't show every extreme that they name: `order`: each of 0 .. 1 appears once.
All inputs are finite; a program needn't handle non-finite values.
Results may differ from the reference program's by a relative error of at most 0.0003.
Values sent between devices are 32-bit elements; how exact they have to be, the bound alone decides.
A program may use at most 64 MiB of HBM per device.

```python
import jax
import jax.numpy as jnp
from jax import lax

W = 4096
NB = 128
NP = 2
LAYERS = 8
N_ROW = 4
N_COL = 16


def draw_subtree_terms(key, part):
    key_off = jax.random.fold_in(key, 11)
    key_diag = jax.random.fold_in(key, 12)
    layer_line = jnp.arange(LAYERS).astype(jnp.float32)
    weights = 1.0 + 2.0 * layer_line / max(LAYERS - 1, 1)
    shares = weights / jnp.sum(weights)
    noise = jax.random.normal(key_off, (LAYERS, W, W), jnp.float32)
    reach = jnp.float32(NB) * 0.5
    off_scale = 0.8 / jnp.sqrt(jnp.float32(W)) * weights / jnp.sqrt(jnp.sum(weights * weights))
    diag = jax.random.uniform(key_diag, (LAYERS, W), jnp.float32, 2.0, 6.0) * shares[:, None]
    eye = jnp.eye(W, dtype=jnp.float32)
    front_line = jnp.arange(W).astype(jnp.float32)
    coupling = 2.0 * jnp.exp(-jnp.abs(front_line[:, None] - front_line[None, :]) / reach)
    front = noise * off_scale[:, None, None] * (1.0 - eye)[None] + diag[:, :, None] * eye[None]
    front = front + shares[:, None, None] * coupling[None]
    store = jnp.arange(W)
    rshard = store // (W // N_ROW)
    rlocal = store % (W // N_ROW)
    rowmap = (rlocal // NB * N_ROW + rshard) * NB + rlocal % NB
    cshard = store // (W // N_COL)
    clocal = store % (W // N_COL)
    colmap = (clocal // NB * N_COL + cshard) * NB + clocal % NB
    return front[:, rowmap][:, :, colmap]


def setup_inputs(seed: int = 0) -> dict:
    seeds = jax.random.split(jax.random.key(seed), 3)
    return {
        "subtree_terms": draw_subtree_terms(jax.random.fold_in(seeds[2], 71), 0),
        "order": jax.random.permutation(seeds[1], NP).astype(jnp.int32),
    }


def invert_block(block):
    size = block.shape[0]
    ident = jnp.eye(size, dtype=jnp.float32)
    index_line = jnp.arange(size)

    def sweep(step, carry):
        mat, inv = carry
        unit = (index_line == step).astype(jnp.float32)
        mat_row = lax.dynamic_index_in_dim(mat, step, 0, keepdims=False)
        inv_row = lax.dynamic_index_in_dim(inv, step, 0, keepdims=False)
        pivot = jnp.sum(mat_row * unit)
        mat_row = mat_row / pivot
        inv_row = inv_row / pivot
        column = jnp.sum(mat * unit[None, :], axis=1) * (1.0 - unit)
        mat = mat - column[:, None] * mat_row[None, :]
        inv = inv - column[:, None] * inv_row[None, :]
        keep = (1.0 - unit)[:, None]
        mat = mat * keep + unit[:, None] * mat_row[None, :]
        inv = inv * keep + unit[:, None] * inv_row[None, :]
        return mat, inv

    mat, inv = lax.fori_loop(0, size, sweep, (block, ident))
    return inv


def storage_of_front(count, groups):
    front_index = jnp.arange(W)
    panel = front_index // NB
    offset = front_index % NB
    return ((panel % groups) * (W // groups) + (panel // groups) * NB + offset).astype(jnp.int32)


def front_of_storage(groups):
    store = jnp.arange(W)
    shard = store // (W // groups)
    local = store % (W // groups)
    return (((local // NB) * groups + shard) * NB + local % NB).astype(jnp.int32)


def reference(subtree_terms, order):
    summed = jnp.sum(subtree_terms, axis=0)
    srow = storage_of_front(W, N_ROW)
    scol = storage_of_front(W, N_COL)
    front = summed[srow][:, scol]
    panel = jnp.arange(W) // NB
    hits = panel[:, None] == order[None, :]
    rank = jnp.where(jnp.any(hits, axis=1), jnp.sum(hits * jnp.arange(NP)[None, :], axis=1), NP)
    hp = lax.Precision.HIGHEST

    def step(k, front):
        p = order[k]
        start = (p * NB).astype(jnp.int32)
        rows_block = lax.dynamic_slice_in_dim(front, start, NB, 0)
        cols_block = lax.dynamic_slice_in_dim(front, start, NB, 1)
        diag_block = lax.dynamic_slice_in_dim(rows_block, start, NB, 1)
        inverse = invert_block(diag_block)
        alive = (rank > k).astype(jnp.float32)
        right = jnp.dot(inverse, rows_block * alive[None, :], precision=hp)
        front = front - jnp.dot(cols_block * alive[:, None], right, precision=hp)
        lower = jnp.dot(cols_block, inverse, precision=hp)
        current = lax.dynamic_slice_in_dim(front, start, NB, 1)
        fresh = jnp.where(alive[:, None] > 0.5, lower, current)
        return lax.dynamic_update_slice_in_dim(front, fresh, start, 1)

    front = lax.fori_loop(0, NP, step, front)
    return front[front_of_storage(N_ROW)][:, front_of_storage(N_COL)]
```

```python
import functools

import jax
import jax.numpy as jnp
from jax import lax
from jax.experimental import pallas as pl
from jax.experimental.pallas import tpu as pltpu
from jax.sharding import PartitionSpec as P

MESH = pl.DeviceIdType.MESH
NB = 128
F32 = jnp.float32
PART = 224
SPLIT_B = (112, 112)
SPLIT_C = (112, 112)


def dev(y, z, x, k):
    y, z, x = lax.rem(y + 8, 4), lax.rem(z + 32, 16), lax.rem(x + 8, 4)
    return (y * 2 + z // 8, x, lax.rem(z, 8) * 2 + k)


def dot(a, b):
    return jnp.dot(a, b, precision=lax.Precision.HIGHEST, preferred_element_type=F32)


def inverse_steps(v, lo, hi):
    n = NB
    lane8 = lax.broadcasted_iota(jnp.int32, (8, n), 1)
    sub8 = lax.broadcasted_iota(jnp.int32, (8, n), 0)
    subc = lax.broadcasted_iota(jnp.int32, (8, 8, n), 1)
    colc = lax.broadcasted_iota(jnp.int32, (8, 8, n), 0)
    lane = lax.broadcasted_iota(jnp.int32, (n, n), 1)
    for b in range(lo, hi):
        o = b * 8
        v0 = v[o : o + 8, :]
        c = jnp.stack([jnp.broadcast_to(v0[:, o + s : o + s + 1], (8, n)) for s in range(8)])
        for s in range(8):
            row = c[:, s : s + 1, :]
            pinv = 1.0 / row[s : s + 1]
            row = jnp.where(colc[:, :1] == s, pinv, row * pinv)
            base = jnp.where(colc == s, 0.0, c)
            c = jnp.where(subc == s, jnp.broadcast_to(row, (8, 8, n)), base - c[s : s + 1] * row)
        eye = (lane8 - o == sub8).astype(F32)
        v0 = jnp.where((lane8 >= o) & (lane8 < o + 8), eye, v0)
        r = c[0] * v0[0:1]
        for s in range(1, 8):
            r = r + c[s] * v0[s : s + 1]
        acc = jnp.where((lane >= o) & (lane < o + 8), 0.0, v)
        for s in range(8):
            acc = acc - v[:, o + s : o + s + 1] * r[s : s + 1]
        parts = [acc[:o]] if o else []
        parts += [r, acc[o + 8 :]] if o + 8 < n else [r]
        v = jnp.concatenate(parts, 0)
    return v


class Chunk:
    def __init__(self, base, stride, off, rows, lo, hi, recv, part, far):
        self.base, self.stride, self.off, self.rows = base, stride, off, rows
        self.cols = slice(lo, hi)
        self.recv, self.part, self.far = recv, part, far

    def at(self, ref, y):
        start = pl.multiple_of(self.base + y * self.stride + self.off, 8)
        return ref.at[pl.ds(start, self.rows), self.cols]

    def xrows(self, ref, k, y):
        start = pl.multiple_of(self.base + y * self.stride + self.off, 8)
        return ref.at[k, pl.ds(start, self.rows)]

    def mine(self, ref, *lead):
        return ref.at[(*lead, slice(self.off, self.off + self.rows))]


def kernel(
    order_ref, t_hbm, o_hbm,
    t, f, u, ra, rb, rc, pa, pb, pc, za, zb, zc, xa, dx, yb, xf, mat,
    in_sem, out_sem, ssem, rsem,
):
    layer, x, col = lax.axis_index("layer"), lax.axis_index("row"), lax.axis_index("col")
    y, zl, k = layer // 2, col // 2, lax.rem(col, 2)
    z = lax.rem(layer, 2) * 8 + zl
    count = [0]
    sends = []

    def new():
        count[0] += 1
        return count[0] - 1

    def copy(i, src, dst, target, j=None):
        return pltpu.make_async_remote_copy(
            src_ref=src, dst_ref=dst, send_sem=ssem.at[i],
            recv_sem=rsem.at[i if j is None else j], device_id=target, device_id_type=MESH,
        )

    def start(c, cond=None):
        if cond is None:
            c.start()
        else:
            pl.when(cond)(c.start)
        sends.append((c, cond))

    a = Chunk(0, 32, 0, 32, 0, 256, ra, pa, za)
    bs, cs, off = [], [], 0
    for n in SPLIT_B:
        bs.append(Chunk(NB, PART, off, n, 0, 128, rb, pb, zb))
        off += n
    off = 0
    for n in SPLIT_C:
        cs.append(Chunk(NB, PART, off, n, 128, 256, rc, pc, zc))
        off += n
    chunks = [a, *bs, *cs]

    loads = [
        pltpu.make_async_copy(t_hbm.at[r, c], t.at[r, c], in_sem.at[i])
        for i, (r, c) in enumerate(
            [
                (slice(0, 128), slice(0, 256)),
                (slice(128, 1024), slice(0, 128)),
                (slice(128, 1024), slice(128, 256)),
            ]
        )
    ]
    for c in loads:
        c.start()

    barrier = pltpu.get_barrier_semaphore()
    peers = [dev(y + i, z, x + j, k) for i in range(4) for j in range(4) if i or j]
    peers += [dev(y, z + d, x, k) for d in (8, 1, 2, 3, 4, -1, -2, -3, -4)]
    peers += [dev(y, z, x, 1 - k)]
    for p in peers:
        pl.semaphore_signal(barrier, inc=1, device_id=p, device_id_type=MESH)
    pl.semaphore_wait(barrier, len(peers))

    rs = {}
    for n, c in enumerate(chunks):
        if n in (0, 1, 1 + len(bs)):
            loads[0 if n == 0 else 1 if n == 1 else 2].wait()
        for d in (1, 3, 2):
            y2 = lax.rem(y + d, 4)
            rs[c, d] = copy(new(), c.at(t, y2), c.mine(c.recv, d - 1), dev(y2, z, x, k))
            start(rs[c, d])
    zx = {}
    for c in chunks:
        for d in (1, 2, 3):
            rs[c, d].wait_recv()
        own, got = c.at(t, y), [c.mine(c.recv, d)[...] for d in range(3)]
        c.mine(c.part)[...] = (own[...] + got[0]) + (got[1] + got[2])
        zx[c] = copy(new(), c.mine(c.part), c.mine(c.far), dev(y, z + 8, x, k))
        start(zx[c])

    ag = {}

    def gather_rows(c):
        zx[c].wait_recv()
        s = c.mine(c.part)[...] + c.mine(c.far)[...]
        c.at(f, y)[...] = s
        return s

    def send_rows(c):
        for d in (1, 3, 2):
            ag[c, d] = copy(new(), c.at(f, y), c.at(f, y), dev(y + d, z, x, k))
            start(ag[c, d])

    s = gather_rows(a)

    @pl.when(zl == 0)
    def _():
        xa[...] = s[:, :128]

    j = new()
    for i, d in enumerate((1, -1, 2, -2, 3, -3, 4)):
        c4 = copy(j if i == 0 else new(), xa, xa, dev(y, z + d, x, k), j)
        start(c4, zl == 0)

    slot = jnp.minimum(x, 2)
    rows_y = pl.ds(pl.multiple_of(y * 32, 8), 32)
    panel = x < 2
    rows_of = {}

    def plane_rows():
        for dxx in (1, 3, 2):
            for dy in range(4):
                rows_of[dxx, dy] = copy(
                    new(), f.at[rows_y], yb.at[jnp.minimum(x, 1), rows_y],
                    dev(y + dy, z, x + dxx, k),
                )
                start(rows_of[dxx, dy], panel)

    send_rows(a)
    plane_rows()

    @pl.when(zl != 0)
    def _():
        copy(j, xa, xa, dev(y, z, x, 1 - k)).wait_recv()

    plane = {}
    for dxx in (0, 1, 3, 2):
        for dy in (0, 1, 3, 2):
            if dxx or dy:
                plane[dxx, dy] = copy(
                    new(), xa, dx.at[slot, k, rows_y], dev(y + dy, z, x + dxx, k)
                )
                start(plane[dxx, dy], panel if dxx else None)
    dx[slot, k, rows_y] = xa[...]

    tree = {}
    xg = {}

    def tree_send(c):
        jt = new()
        here = c.xrows(xf, k, y)
        tree[c] = copy(jt, here, here, dev(y, z, x, 1 - k))
        idx = [jt, new(), new(), new()]
        for i, d in zip(idx, (2, -2, 1, -1)):
            start(copy(i, here, here, dev(y, z + d, x, k), jt), zl == 0)
        return idx

    def tree_pass(c, idx):
        here = c.xrows(xf, k, y)
        jt = idx[0]

        @pl.when(zl != 0)
        def _():
            tree[c].wait_recv()

        start(copy(idx[0], here, here, dev(y, z + 2, x, k), jt), zl == 2)
        start(copy(idx[1], here, here, dev(y, z + 1, x, k), jt), zl == 2)
        start(copy(idx[0], here, here, dev(y, z - 1, x, k), jt), zl == 6)
        for d in (1, 3, 2):
            xg[c, d] = copy(new(), here, here, dev(y + d, z, x, k))
            start(xg[c, d])

    tree_idx = {}

    def columns(c):
        s = gather_rows(c)

        @pl.when(zl == 0)
        def _():
            c.xrows(xf, k, y)[...] = s

        tree_idx[c] = tree_send(c)
        send_rows(c)

    columns(bs[0])

    for dxx in range(4):
        for dy in range(4):
            if dxx or dy:
                if dxx:
                    cond = lax.rem(x - dxx + 4, 4) < 2
                    pl.when(cond)(plane[dxx, dy].wait_recv)
                else:
                    plane[dxx, dy].wait_recv()
    sib = copy(new(), dx.at[0:2, k], dx.at[0:2, k], dev(y, z, x, 1 - k))
    start(sib)
    sib2 = copy(new(), dx.at[2, k], dx.at[2, k], dev(y, z, x, 1 - k))
    start(sib2, x >= 2)
    sib.wait_recv()

    first = order_ref[0]
    swapped = jnp.full((NB, NB), first, jnp.int32) == 1
    d00, d01, d10, d11 = dx[0, 0], dx[0, 1], dx[1, 0], dx[1, 1]
    dpp, dqq = jnp.where(swapped, d11, d00), jnp.where(swapped, d00, d11)
    dpq, dqp = jnp.where(swapped, d10, d01), jnp.where(swapped, d01, d10)

    mat[0] = inverse_steps(dpp, 0, 8)
    tree_pass(bs[0], tree_idx[bs[0]])
    for c in bs[1:]:
        columns(c)
    mat[0] = inverse_steps(mat[0], 8, 16)
    pinv = mat[0]
    w = dot(pinv, dpq)
    v = dot(dqp, pinv)
    mat[1] = dqq - dot(dqp, w)
    for c in bs[1:]:
        tree_pass(c, tree_idx[c])
    mat[1] = inverse_steps(mat[1], 0, 8)
    for c in cs[:-1]:
        gather_rows(c)
        send_rows(c)
    mat[1] = inverse_steps(mat[1], 8, 16)
    for c in cs[-1:]:
        gather_rows(c)
        send_rows(c)
    qinv = mat[1]

    for d in (1, 2, 3):
        ag[a, d].wait_recv()
    for (dxx, dy), c in rows_of.items():
        pl.when(lax.rem(x - dxx + 4, 4) < 2)(c.wait_recv)
    for i in range(2):

        @pl.when(x == i)
        def _(i=i):
            yb[i] = f[0:NB, :]

    def full(value):
        return jnp.full((NB, 256), value, jnp.int32)

    wide = full(first) == 1
    y0, y1 = yb[0], yb[1]
    yp, yq = jnp.where(wide, y1, y0), jnp.where(wide, y0, y1)
    tp = dot(pinv, yp)
    gq = dot(qinv, yq - dot(v, yp))
    gp = tp - dot(w, gq)
    left = lax.broadcasted_iota(jnp.int32, (NB, 256), 1) < NB
    here = left & (full(zl) == 0)
    is_p = here & (full(first) == full(k))
    is_q = here & (full(first) != full(k))
    zero = jnp.zeros((NB, NB), F32)
    pad_p = jnp.concatenate([pinv, zero], 1)
    pad_q = jnp.concatenate([qinv, zero], 1)
    pad_wq = jnp.concatenate([dot(w, qinv), zero], 1)
    gp = jnp.where(is_p, -pad_p, jnp.where(is_q, pad_wq, gp))
    gq = jnp.where(is_p, 0.0, jnp.where(is_q, -pad_q, gq))
    row_p = full(first) == full(x)
    row_q = (full(x) < 2) & (full(first) != full(x))
    gp0 = jnp.where(row_p, 0.0, jnp.where(row_q, jnp.where(is_p, -pad_p, tp), gp))
    gq0 = jnp.where(row_p | row_q, 0.0, gq)
    drop0 = (is_p & ~row_p) | (is_q & ~row_p & ~row_q)
    drop = is_p | is_q

    def stacked(p, q):
        return jnp.concatenate([jnp.where(wide, q, p), jnp.where(wide, p, q)], 0)

    g0, g = stacked(gp0, gq0), stacked(gp, gq)

    pl.when(x >= 2)(sib2.wait_recv)
    x0 = jnp.concatenate([dx[slot, 0], dx[slot, 1]], 1)
    u[0:NB, :] = jnp.where(drop0, 0.0, f[0:NB, :]) - dot(x0, g0)

    for c in xg.values():
        c.wait_recv()
    xs = copy(new(), xf.at[k, NB:], xf.at[k, NB:], dev(y, z, x, 1 - k))
    start(xs)
    xs.wait_recv()
    for n in range(7):
        r = slice(NB + n * NB, 2 * NB + n * NB)
        u[r, :] = dot(jnp.concatenate([xf[0, r], xf[1, r]], 1), g)
    for c in chunks[1:]:
        for d in (1, 2, 3):
            ag[c, d].wait_recv()
    for n in range(7):
        r = slice(NB + n * NB, 2 * NB + n * NB)
        u[r, :] = jnp.where(drop, 0.0, f[r, :]) - u[r, :]
    out = pltpu.make_async_copy(u, o_hbm, out_sem.at[0])
    out.start()
    for c, cond in sends:
        if cond is None:
            c.wait_send()
        else:
            pl.when(cond)(c.wait_send)
    out.wait()


def solution(mesh):
    rows, cols = 1024, 256

    def body(terms, order):
        vm = lambda *s: pltpu.VMEM(s, F32)
        return pl.pallas_call(
            kernel,
            out_shape=jax.ShapeDtypeStruct((rows, cols), F32),
            in_specs=[
                pl.BlockSpec(memory_space=pltpu.SMEM),
                pl.BlockSpec(memory_space=pl.ANY),
            ],
            out_specs=pl.BlockSpec(memory_space=pl.ANY),
            scratch_shapes=[
                vm(rows, cols), vm(rows, cols), vm(rows, cols),
                vm(3, 32, 256), vm(3, PART, 128), vm(3, PART, 128),
                vm(32, 256), vm(PART, 128), vm(PART, 128),
                vm(32, 256), vm(PART, 128), vm(PART, 128),
                vm(32, 128), vm(3, 2, 128, 128), vm(2, 128, 256), vm(2, rows, 128), vm(2, 128, 128),
                pltpu.SemaphoreType.DMA((3,)),
                pltpu.SemaphoreType.DMA((1,)),
                pltpu.SemaphoreType.DMA((128,)),
                pltpu.SemaphoreType.DMA((128,)),
            ],
            compiler_params=pltpu.CompilerParams(collective_id=0, has_side_effects=True),
            name="front",
        )(order, terms.reshape(rows, cols))

    return jax.shard_map(
        body,
        mesh=mesh,
        in_specs=(P("layer", "row", "col"), P()),
        out_specs=P("row", "col"),
        check_vma=False,
    )
```

```python
import functools

import jax
import jax.numpy as jnp
from jax import lax
from jax.experimental import pallas as pl
from jax.experimental.pallas import tpu as pltpu
from jax.sharding import PartitionSpec as P

MESH = pl.DeviceIdType.MESH
NB = 128
F32 = jnp.float32
PART = 224
SPLIT = (112, 112)


def dev(y, z, x, k):
    y, z, x = lax.rem(y + 8, 4), lax.rem(z + 32, 16), lax.rem(x + 8, 4)
    return (y * 2 + z // 8, x, lax.rem(z, 8) * 2 + k)


def dot(a, b):
    return jnp.dot(a, b, precision=lax.Precision.HIGHEST, preferred_element_type=F32)


def inverse_steps(v, lo, hi):
    n = NB
    lane8 = lax.broadcasted_iota(jnp.int32, (8, n), 1)
    sub8 = lax.broadcasted_iota(jnp.int32, (8, n), 0)
    subc = lax.broadcasted_iota(jnp.int32, (8, 8, n), 1)
    colc = lax.broadcasted_iota(jnp.int32, (8, 8, n), 0)
    lane = lax.broadcasted_iota(jnp.int32, (n, n), 1)
    for b in range(lo, hi):
        o = b * 8
        v0 = v[o : o + 8, :]
        c = jnp.stack([jnp.broadcast_to(v0[:, o + s : o + s + 1], (8, n)) for s in range(8)])
        for s in range(8):
            row = c[:, s : s + 1, :]
            pinv = 1.0 / row[s : s + 1]
            row = jnp.where(colc[:, :1] == s, pinv, row * pinv)
            base = jnp.where(colc == s, 0.0, c)
            c = jnp.where(subc == s, jnp.broadcast_to(row, (8, 8, n)), base - c[s : s + 1] * row)
        eye = (lane8 - o == sub8).astype(F32)
        v0 = jnp.where((lane8 >= o) & (lane8 < o + 8), eye, v0)
        r = c[0] * v0[0:1]
        for s in range(1, 8):
            r = r + c[s] * v0[s : s + 1]
        acc = jnp.where((lane >= o) & (lane < o + 8), 0.0, v)
        for s in range(8):
            acc = acc - v[:, o + s : o + s + 1] * r[s : s + 1]
        parts = [acc[:o]] if o else []
        parts += [r, acc[o + 8 :]] if o + 8 < n else [r]
        v = jnp.concatenate(parts, 0)
    return v


class Chunk:
    def __init__(self, base, stride, off, rows, lo, hi, recv, part, far):
        self.base, self.stride, self.off, self.rows = base, stride, off, rows
        self.cols = slice(lo, hi)
        self.sub = slice(off, off + rows)
        self.recv, self.part, self.far = recv, part, far

    def at(self, ref, y):
        start = pl.multiple_of(self.base + y * self.stride + self.off, 8)
        return ref.at[pl.ds(start, self.rows), self.cols]

    def mine(self, ref, *lead):
        return ref.at[(*lead, self.sub)]


def kernel(
    order_ref, t_hbm, o_hbm,
    t, f, u, ra, rb, rc, pa, pb, pc, za, zb, zc, xh, xa, dx, yb, xf, mat,
    in_sem, out_sem, ssem, rsem,
):
    layer, x, col = lax.axis_index("layer"), lax.axis_index("row"), lax.axis_index("col")
    y, zl, k = layer // 2, col // 2, lax.rem(col, 2)
    zh = lax.rem(layer, 2)
    z = zh * 8 + zl
    source, relay = zl == 0, (zl == 2) | (zl == 6)
    other = dev(y, z, x, 1 - k)
    count = [0]
    sends = []

    def new():
        count[0] += 1
        return count[0] - 1

    def copy(i, src, dst, target, j=None):
        return pltpu.make_async_remote_copy(
            src_ref=src, dst_ref=dst, send_sem=ssem.at[i],
            recv_sem=rsem.at[i if j is None else j], device_id=target, device_id_type=MESH,
        )

    def start(c, cond=None):
        if cond is None:
            c.start()
        else:
            pl.when(cond)(c.start)
        sends.append((c, cond))

    a = Chunk(0, 32, 0, 32, 0, 256, ra, pa, za)
    bs, cs, off = [], [], 0
    for n in SPLIT:
        bs.append(Chunk(NB, PART, off, n, 0, 128, rb, pb, zb))
        cs.append(Chunk(NB, PART, off, n, 128, 256, rc, pc, zc))
        off += n
    chunks = [a, *bs, *cs]

    loads = [
        pltpu.make_async_copy(t_hbm.at[r, c], t.at[r, c], in_sem.at[i])
        for i, (r, c) in enumerate(
            [
                (slice(0, 128), slice(0, 256)),
                (slice(128, 1024), slice(0, 128)),
                (slice(128, 1024), slice(128, 256)),
            ]
        )
    ]
    for c in loads:
        c.start()

    barrier = pltpu.get_barrier_semaphore()
    peers = [dev(y + i, z, x + j, k) for i in range(4) for j in range(4) if i or j]
    peers += [dev(y, z + d, x, k) for d in range(1, 16)]
    peers += [other]
    for p in peers:
        pl.semaphore_signal(barrier, inc=1, device_id=p, device_id_type=MESH)
    pl.semaphore_wait(barrier, len(peers))

    rs, zx = {}, {}
    for n, c in enumerate(chunks):
        if n in (0, 1, 1 + len(bs)):
            loads[0 if n == 0 else 1 if n == 1 else 2].wait()
        for d in (1, 3, 2):
            y2 = lax.rem(y + d, 4)
            rs[c, d] = copy(new(), c.at(t, y2), c.mine(c.recv, d - 1), dev(y2, z, x, k))
            start(rs[c, d])

    def half_sum(c):
        for d in (1, 2, 3):
            rs[c, d].wait_recv()
        own, got = c.at(t, y), [c.mine(c.recv, d)[...] for d in range(3)]
        c.mine(c.part)[...] = (own[...] + got[0]) + (got[1] + got[2])
        zx[c] = copy(new(), c.mine(c.part), c.mine(c.far), dev(y, z + 8, x, k))
        sends.append((zx[c], None))

    def full_sum(c):
        zx[c].wait_recv()
        return c.mine(c.part)[...] + c.mine(c.far)[...]

    half_sum(a)
    xhalf = {}
    for d in (1, 15, 2, 14, 3, 13, 4, 12, 5, 11, 6, 10, 7, 9, 8):
        i = new()
        if not xhalf:
            xhalf[0], xhalf[1] = i, new()
        for h in range(2):
            c = copy(i, pa.at[:, :128], xh.at[h], dev(y, z + d, x, k), xhalf[h])
            start(c, source & (zh == h))
    panel = x < 2
    plain, inner = jnp.logical_not(panel), jnp.logical_not(source)
    leaf = jnp.logical_not(source | relay)
    pl.when(plain & inner)(zx[a].start)
    half_sum(bs[0])
    pl.when(panel & inner)(zx[a].start)
    pl.when(plain)(zx[bs[0]].start)
    for c in bs[1:]:
        half_sum(c)
    pl.when(panel)(zx[bs[0]].start)
    for c in bs[1:]:
        zx[c].start()
    pl.when(source)(zx[a].start)
    half_sum(cs[0])
    pl.when(leaf)(zx[cs[0]].start)

    slot = jnp.minimum(x, 2)
    rows_y = pl.ds(pl.multiple_of(y * 32, 8), 32)
    plane = {(i, j): new() for i in (0, 1, 3, 2) for j in (0, 1, 3, 2) if i or j}

    def across(i, j):
        return copy(plane[i, j], xa, dx.at[slot, k, rows_y], dev(y + j, z, x + i, k))

    def columns(cond):
        for h in range(2):

            @pl.when(cond & source & (zh == h))
            def _(h=h):
                xh[h] = pa[:, :128]

            @pl.when(cond & jnp.logical_not(source & (zh == h)))
            def _(h=h):
                copy(xhalf[h], xh.at[h], xh.at[h], other).wait_recv()

        @pl.when(cond)
        def _():
            xa[...] = xh[0] + xh[1]
            dx[slot, k, rows_y] = xa[...]

        for i, j in plane:
            if cond is panel or not i:
                start(across(i, j), cond)

    columns(panel)
    for c in cs[1:]:
        half_sum(c)
        pl.when(leaf)(zx[c].start)

    f[rows_y, :] = full_sum(a)
    ag = {}
    for d in (1, 3, 2):
        ag[a, d] = copy(new(), f.at[rows_y], f.at[rows_y], dev(y + d, z, x, k))
        start(ag[a, d])
    rows_of = {}
    for dxx in (1, 3, 2):
        for dy in range(4):
            rows_of[dxx, dy] = copy(
                new(), f.at[rows_y], yb.at[jnp.minimum(x, 1), rows_y],
                dev(y + dy, z, x + dxx, k),
            )
            start(rows_of[dxx, dy], panel)

    branch, xg = {}, {}

    def spread(c, cond):
        for d in (1, 3, 2):
            pl.when(cond)(xg[c, d].start)

    def gather(c):
        zx[c].wait_recv()
        total = c.mine(c.part)[...] + c.mine(c.far)[...]
        if c in bs:
            here = c.mine(xf, k, y)
            branch[c] = [new() for _ in range(4)]
            for d in (1, 3, 2):
                xg[c, d] = copy(new(), here, here, dev(y + d, z, x, k))
                sends.append((xg[c, d], None))

            @pl.when(source)
            def _():
                here[...] = total

            for i, d in zip(branch[c], (2, -2, 1, -1)):
                start(copy(i, here, here, dev(y, z + d, x, k), branch[c][0]), source)
            spread(c, source)
            total = jnp.where(jnp.full((c.rows, 128), zl, jnp.int32) == 0, 0.0, total)
        c.at(f, y)[...] = total
        for d in (1, 3, 2):
            ag[c, d] = copy(new(), c.at(f, y), c.at(f, y), dev(y + d, z, x, k))
            start(ag[c, d])

    def pass_on(c, cond):
        here = c.mine(xf, k, y)
        i, i2 = branch[c][:2]

        @pl.when(cond)
        def _():
            copy(i, here, here, other).wait_recv()

        if cond is relay:
            start(copy(i, here, here, dev(y, z + 2, x, k), i), zl == 2)
            start(copy(i2, here, here, dev(y, z + 1, x, k), i), zl == 2)
            start(copy(i, here, here, dev(y, z - 1, x, k), i), zl == 6)
        spread(c, cond)

    for i, j in plane:
        pl.when(lax.rem(x - i + 4, 4) < 2)(across(i, j).wait_recv)
    gather(bs[0])
    pl.when(source)(zx[cs[0]].start)
    sib = copy(new(), dx.at[0:2, k], dx.at[0:2, k], other)
    start(sib)
    sib2 = copy(new(), dx.at[2, k], dx.at[2, k], other)
    sib.wait_recv()

    first = order_ref[0]
    swapped = jnp.full((NB, NB), first, jnp.int32) == 1
    d00, d01, d10, d11 = dx[0, 0], dx[0, 1], dx[1, 0], dx[1, 1]
    dpp, dqq = jnp.where(swapped, d11, d00), jnp.where(swapped, d00, d11)
    dpq, dqp = jnp.where(swapped, d10, d01), jnp.where(swapped, d01, d10)

    mat[0] = inverse_steps(dpp, 0, 8)
    pass_on(bs[0], relay)
    pl.when(relay)(zx[cs[0]].start)
    for c in bs[1:]:
        gather(c)
    for c in cs[1:]:
        pl.when(source)(zx[c].start)
    mat[0] = inverse_steps(mat[0], 8, 16)
    pinv = mat[0]
    w = dot(pinv, dpq)
    v = dot(dqp, pinv)
    mat[1] = dqq - dot(dqp, w)
    mat[1] = inverse_steps(mat[1], 0, 8)
    for c in bs[1:]:
        pass_on(c, relay)
    for c in cs[1:]:
        pl.when(relay)(zx[c].start)
    mat[1] = inverse_steps(mat[1], 8, 16)
    qinv = mat[1]
    columns(plain)

    for d in (1, 2, 3):
        ag[a, d].wait_recv()
    for (dxx, dy), c in rows_of.items():
        pl.when(lax.rem(x - dxx + 4, 4) < 2)(c.wait_recv)
    for i in range(2):

        @pl.when(x == i)
        def _(i=i):
            yb[i] = f[0:NB, :]

    def full(value):
        return jnp.full((NB, 256), value, jnp.int32)

    wide = full(first) == 1
    y0, y1 = yb[0], yb[1]
    yp, yq = jnp.where(wide, y1, y0), jnp.where(wide, y0, y1)
    tp = dot(pinv, yp)
    gq = dot(qinv, yq - dot(v, yp))
    gp = tp - dot(w, gq)
    left = lax.broadcasted_iota(jnp.int32, (NB, 256), 1) < NB
    here = left & (full(zl) == 0)
    is_p = here & (full(first) == full(k))
    is_q = here & (full(first) != full(k))
    zero = jnp.zeros((NB, NB), F32)
    pad_p = jnp.concatenate([pinv, zero], 1)
    pad_q = jnp.concatenate([qinv, zero], 1)
    pad_wq = jnp.concatenate([dot(w, qinv), zero], 1)
    gp = jnp.where(is_p, -pad_p, jnp.where(is_q, pad_wq, gp))
    gq = jnp.where(is_p, 0.0, jnp.where(is_q, -pad_q, gq))
    row_p = full(first) == full(x)
    row_q = (full(x) < 2) & (full(first) != full(x))
    gp0 = jnp.where(row_p, 0.0, jnp.where(row_q, jnp.where(is_p, -pad_p, tp), gp))
    gq0 = jnp.where(row_p | row_q, 0.0, gq)
    drop0 = (is_p & ~row_p) | (is_q & ~row_p & ~row_q)

    def stacked(p, q):
        return jnp.concatenate([jnp.where(wide, q, p), jnp.where(wide, p, q)], 0)

    g0, g = stacked(gp0, gq0), stacked(gp, gq)

    for j in range(1, 4):
        pl.when(plain)(across(0, j).wait_recv)
    start(sib2, plain)
    for c in cs[:-1]:
        gather(c)
    pl.when(plain)(sib2.wait_recv)
    x0 = jnp.concatenate([dx[slot, 0], dx[slot, 1]], 1)
    u[0:NB, :] = jnp.where(drop0, 0.0, f[0:NB, :]) - dot(x0, g0)
    outs = []

    def put(r, cols):
        outs.append(pltpu.make_async_copy(u.at[r, cols], o_hbm.at[r, cols], out_sem.at[len(outs)]))
        outs[-1].start()

    put(slice(0, NB), slice(0, 256))
    side = {}
    pass_on(bs[0], leaf)
    gather(cs[-1])
    for c in bs[1:]:
        pass_on(c, leaf)
    for c in bs:
        for d in (1, 2, 3):
            xg[c, d].wait_recv()
        here = xf.at[k, :, c.sub]
        side[c] = copy(new(), here, here, other)
        start(side[c])
    for c in bs:
        side[c].wait_recv()
    for i in range(4):
        u[NB + i * PART : NB + (i + 1) * PART, :] = dot(
            jnp.concatenate([xf[0, i], xf[1, i]], 1), g
        )
    for c in chunks[1:]:
        for d in (1, 2, 3):
            ag[c, d].wait_recv()
        for i in range(4):
            r = slice(NB + i * PART + c.off, NB + i * PART + c.off + c.rows)
            u[r, c.cols] = f[r, c.cols] - u[r, c.cols]
            put(r, c.cols)
    for c, cond in sends:
        if cond is None:
            c.wait_send()
        else:
            pl.when(cond)(c.wait_send)
    for c in outs:
        c.wait()


def solution(mesh):
    rows, cols = 1024, 256

    def body(terms, order):
        vm = lambda *s: pltpu.VMEM(s, F32)
        return pl.pallas_call(
            kernel,
            out_shape=jax.ShapeDtypeStruct((rows, cols), F32),
            in_specs=[
                pl.BlockSpec(memory_space=pltpu.SMEM),
                pl.BlockSpec(memory_space=pl.ANY),
            ],
            out_specs=pl.BlockSpec(memory_space=pl.ANY),
            scratch_shapes=[
                vm(rows, cols), vm(rows, cols), vm(rows, cols),
                vm(3, 32, 256), vm(3, PART, 128), vm(3, PART, 128),
                vm(32, 256), vm(PART, 128), vm(PART, 128),
                vm(32, 256), vm(PART, 128), vm(PART, 128),
                vm(2, 32, 128), vm(32, 128), vm(3, 2, 128, 128), vm(2, 128, 256),
                vm(2, 4, PART, 128), vm(2, 128, 128),
                pltpu.SemaphoreType.DMA((3,)),
                pltpu.SemaphoreType.DMA((1 + 8 * len(SPLIT),)),
                pltpu.SemaphoreType.DMA((128,)),
                pltpu.SemaphoreType.DMA((128,)),
            ],
            compiler_params=pltpu.CompilerParams(collective_id=0, has_side_effects=True),
            name="front",
        )(order, terms.reshape(rows, cols))

    return jax.shard_map(
        body,
        mesh=mesh,
        in_specs=(P("layer", "row", "col"), P()),
        out_specs=P("row", "col"),
        check_vma=False,
    )
```

```python
import functools

import jax
import jax.numpy as jnp
from jax import lax
from jax.experimental import pallas as pl
from jax.experimental.pallas import tpu as pltpu
from jax.sharding import PartitionSpec as P

MESH = pl.DeviceIdType.MESH
NB = 128
F32 = jnp.float32
PART = 224
SPLIT = (112, 112)


def dev(y, z, x, k):
    y, z, x = lax.rem(y + 8, 4), lax.rem(z + 32, 16), lax.rem(x + 8, 4)
    return (y * 2 + z // 8, x, lax.rem(z, 8) * 2 + k)


def dot(a, b):
    return jnp.dot(a, b, precision=lax.Precision.HIGHEST, preferred_element_type=F32)


def inverse_steps(v, lo, hi):
    n = NB
    lane8 = lax.broadcasted_iota(jnp.int32, (8, n), 1)
    sub8 = lax.broadcasted_iota(jnp.int32, (8, n), 0)
    subc = lax.broadcasted_iota(jnp.int32, (8, 8, n), 1)
    colc = lax.broadcasted_iota(jnp.int32, (8, 8, n), 0)
    lane = lax.broadcasted_iota(jnp.int32, (n, n), 1)
    for b in range(lo, hi):
        o = b * 8
        v0 = v[o : o + 8, :]
        c = jnp.stack([jnp.broadcast_to(v0[:, o + s : o + s + 1], (8, n)) for s in range(8)])
        for s in range(8):
            row = c[:, s : s + 1, :]
            pinv = 1.0 / row[s : s + 1]
            row = jnp.where(colc[:, :1] == s, pinv, row * pinv)
            base = jnp.where(colc == s, 0.0, c)
            c = jnp.where(subc == s, jnp.broadcast_to(row, (8, 8, n)), base - c[s : s + 1] * row)
        eye = (lane8 - o == sub8).astype(F32)
        v0 = jnp.where((lane8 >= o) & (lane8 < o + 8), eye, v0)
        r = c[0] * v0[0:1]
        for s in range(1, 8):
            r = r + c[s] * v0[s : s + 1]
        acc = jnp.where((lane >= o) & (lane < o + 8), 0.0, v)
        for s in range(8):
            acc = acc - v[:, o + s : o + s + 1] * r[s : s + 1]
        parts = [acc[:o]] if o else []
        parts += [r, acc[o + 8 :]] if o + 8 < n else [r]
        v = jnp.concatenate(parts, 0)
    return v


class Chunk:
    def __init__(self, base, stride, off, rows, lo, hi, recv, part, far):
        self.base, self.stride, self.off, self.rows = base, stride, off, rows
        self.cols = slice(lo, hi)
        self.sub = slice(off, off + rows)
        self.recv, self.part, self.far = recv, part, far

    def at(self, ref, y):
        start = pl.multiple_of(self.base + y * self.stride + self.off, 8)
        return ref.at[pl.ds(start, self.rows), self.cols]

    def mine(self, ref, *lead):
        return ref.at[(*lead, self.sub)]


def kernel(
    order_hbm, t_hbm, u,
    order_ref, t, f, ra, rb, rc, pa, pb, pc, za, zb, zc, xh, xa, dx, yb, xf, mat,
    in_sem, ssem, rsem,
):
    layer, x, col = lax.axis_index("layer"), lax.axis_index("row"), lax.axis_index("col")
    y, zl, k = layer // 2, col // 2, lax.rem(col, 2)
    zh = lax.rem(layer, 2)
    z = zh * 8 + zl
    source, relay = zl == 0, (zl == 2) | (zl == 6)
    other = dev(y, z, x, 1 - k)
    count = [0]
    sends = []

    def new():
        count[0] += 1
        return count[0] - 1

    def copy(i, src, dst, target, j=None):
        return pltpu.make_async_remote_copy(
            src_ref=src, dst_ref=dst, send_sem=ssem.at[i],
            recv_sem=rsem.at[i if j is None else j], device_id=target, device_id_type=MESH,
        )

    def start(c, cond=None):
        if cond is None:
            c.start()
        else:
            pl.when(cond)(c.start)
        sends.append((c, cond))

    a = Chunk(0, 32, 0, 32, 0, 256, ra, pa, za)
    bs, cs, off = [], [], 0
    for n in SPLIT:
        bs.append(Chunk(NB, PART, off, n, 0, 128, rb, pb, zb))
        cs.append(Chunk(NB, PART, off, n, 128, 256, rc, pc, zc))
        off += n
    chunks = [a, *bs, *cs]

    loads = [
        pltpu.make_async_copy(t_hbm.at[r, c], t.at[r, c], in_sem.at[i])
        for i, (r, c) in enumerate(
            [
                (slice(0, 128), slice(0, 256)),
                (slice(128, 1024), slice(0, 128)),
                (slice(128, 1024), slice(128, 256)),
            ]
        )
    ]
    loads.append(pltpu.make_async_copy(order_hbm, order_ref, in_sem.at[3]))
    for c in loads:
        c.start()

    barrier = pltpu.get_barrier_semaphore()
    peers = [dev(y + i, z, x + j, k) for i in range(4) for j in range(4) if i or j]
    peers += [dev(y, z + d, x, k) for d in range(1, 16)]
    peers += [other]
    for p in peers:
        pl.semaphore_signal(barrier, inc=1, device_id=p, device_id_type=MESH)
    pl.semaphore_wait(barrier, len(peers))

    rs, zx = {}, {}
    for n, c in enumerate(chunks):
        if n in (0, 1, 1 + len(bs)):
            loads[0 if n == 0 else 1 if n == 1 else 2].wait()
        for d in (1, 3, 2):
            y2 = lax.rem(y + d, 4)
            rs[c, d] = copy(new(), c.at(t, y2), c.mine(c.recv, d - 1), dev(y2, z, x, k))
            start(rs[c, d])

    def half_sum(c):
        for d in (1, 2, 3):
            rs[c, d].wait_recv()
        own, got = c.at(t, y), [c.mine(c.recv, d)[...] for d in range(3)]
        c.mine(c.part)[...] = (own[...] + got[0]) + (got[1] + got[2])
        zx[c] = copy(new(), c.mine(c.part), c.mine(c.far), dev(y, z + 8, x, k))
        sends.append((zx[c], None))

    def full_sum(c):
        zx[c].wait_recv()
        return c.mine(c.part)[...] + c.mine(c.far)[...]

    half_sum(a)
    xhalf = {}
    for d in (1, 15, 2, 14, 3, 13, 4, 12, 5, 11, 6, 10, 7, 9, 8):
        i = new()
        if not xhalf:
            xhalf[0], xhalf[1] = i, new()
        for h in range(2):
            c = copy(i, pa.at[:, :128], xh.at[h], dev(y, z + d, x, k), xhalf[h])
            start(c, source & (zh == h))
    panel = x < 2
    plain, inner = jnp.logical_not(panel), jnp.logical_not(source)
    leaf = jnp.logical_not(source | relay)
    far = (zl == 3) | (zl == 4) | (zl == 5)
    near = jnp.logical_not(source | far)
    pl.when(plain)(zx[a].start)
    half_sum(bs[0])
    pl.when(panel)(zx[a].start)
    pl.when(plain)(zx[bs[0]].start)
    for c in bs[1:]:
        half_sum(c)
    pl.when(panel)(zx[bs[0]].start)
    for c in bs[1:]:
        zx[c].start()
    half_sum(cs[0])
    pl.when(inner)(zx[cs[0]].start)

    slot = jnp.minimum(x, 2)
    rows_y = pl.ds(pl.multiple_of(y * 32, 8), 32)
    plane = {(i, j): new() for i in (0, 1, 3, 2) for j in (0, 1, 3, 2) if i or j}

    def across(i, j):
        return copy(plane[i, j], xa, dx.at[slot, k, rows_y], dev(y + j, z, x + i, k))

    def columns(cond):
        for h in range(2):

            @pl.when(cond & source & (zh == h))
            def _(h=h):
                xh[h] = pa[:, :128]

            @pl.when(cond & jnp.logical_not(source & (zh == h)))
            def _(h=h):
                copy(xhalf[h], xh.at[h], xh.at[h], other).wait_recv()

        @pl.when(cond)
        def _():
            xa[...] = xh[0] + xh[1]
            dx[slot, k, rows_y] = xa[...]

        for i, j in plane:
            if cond is panel or not i:
                start(across(i, j), cond)

    columns(panel)
    for c in cs[1:]:
        half_sum(c)
        pl.when(leaf)(zx[c].start)

    f[rows_y, :] = full_sum(a)
    ag = {}
    for d in (1, 3, 2):
        ag[a, d] = copy(new(), f.at[rows_y], f.at[rows_y], dev(y + d, z, x, k))
        start(ag[a, d])
    rows_of = {}
    for dxx in (1, 3, 2):
        for dy in range(4):
            rows_of[dxx, dy] = copy(
                new(), f.at[rows_y], yb.at[jnp.minimum(x, 1), rows_y],
                dev(y + dy, z, x + dxx, k),
            )
            start(rows_of[dxx, dy], panel)

    branch, xg = {}, {}

    def spread(c, cond):
        for d in (1, 3, 2):
            pl.when(cond)(xg[c, d].start)

    def gather(c):
        zx[c].wait_recv()
        total = c.mine(c.part)[...] + c.mine(c.far)[...]
        if c in bs:
            here = c.mine(xf, k, y)
            branch[c] = [new() for _ in range(4)]
            for d in (1, 3, 2):
                xg[c, d] = copy(new(), here, here, dev(y + d, z, x, k))
                sends.append((xg[c, d], None))

            @pl.when(source)
            def _():
                here[...] = total

            for i, d in zip(branch[c], (2, -2, 1, -1)):
                start(copy(i, here, here, dev(y, z + d, x, k), branch[c][0]), source)
            spread(c, source)
            total = jnp.where(jnp.full((c.rows, 128), zl, jnp.int32) == 0, 0.0, total)
        c.at(f, y)[...] = total
        for d in (1, 3, 2):
            ag[c, d] = copy(new(), c.at(f, y), c.at(f, y), dev(y + d, z, x, k))
            start(ag[c, d])

    def pass_on(c, cond):
        here = c.mine(xf, k, y)
        i, i2 = branch[c][:2]

        @pl.when(cond)
        def _():
            copy(i, here, here, other).wait_recv()

        if cond is near:
            start(copy(i, here, here, dev(y, z + 2, x, k), i), zl == 2)
            start(copy(i2, here, here, dev(y, z + 1, x, k), i), zl == 2)
            start(copy(i, here, here, dev(y, z - 1, x, k), i), zl == 6)
        spread(c, cond)

    for i, j in plane:
        pl.when(lax.rem(x - i + 4, 4) < 2)(across(i, j).wait_recv)
    sib = copy(new(), dx.at[0:2, k], dx.at[0:2, k], other)
    start(sib)
    sib2 = copy(new(), dx.at[2, k], dx.at[2, k], other)
    gather(bs[0])
    pl.when(source)(zx[cs[0]].start)
    sib.wait_recv()

    loads[3].wait()
    first = order_ref[0]
    swapped = jnp.full((NB, NB), first, jnp.int32) == 1
    d00, d01, d10, d11 = dx[0, 0], dx[0, 1], dx[1, 0], dx[1, 1]
    dpp, dqq = jnp.where(swapped, d11, d00), jnp.where(swapped, d00, d11)
    dpq, dqp = jnp.where(swapped, d10, d01), jnp.where(swapped, d01, d10)

    mat[0] = inverse_steps(dpp, 0, 8)
    pass_on(bs[0], near)
    for c in cs[1:]:
        pl.when(relay)(zx[c].start)
    for c in bs[1:]:
        gather(c)
    for c in cs[1:]:
        pl.when(source)(zx[c].start)
    mat[0] = inverse_steps(mat[0], 8, 16)
    pinv = mat[0]
    w = dot(pinv, dpq)
    v = dot(dqp, pinv)
    mat[1] = dqq - dot(dqp, w)
    mat[1] = inverse_steps(mat[1], 0, 8)
    for c in bs[1:]:
        pass_on(c, near)
    mat[1] = inverse_steps(mat[1], 8, 16)
    qinv = mat[1]
    pass_on(bs[0], far)
    columns(plain)

    for d in (1, 2, 3):
        ag[a, d].wait_recv()
    for (dxx, dy), c in rows_of.items():
        pl.when(lax.rem(x - dxx + 4, 4) < 2)(c.wait_recv)
    for i in range(2):

        @pl.when(x == i)
        def _(i=i):
            yb[i] = f[0:NB, :]

    def full(value):
        return jnp.full((NB, 256), value, jnp.int32)

    wide = full(first) == 1
    y0, y1 = yb[0], yb[1]
    yp, yq = jnp.where(wide, y1, y0), jnp.where(wide, y0, y1)
    tp = dot(pinv, yp)
    gq = dot(qinv, yq - dot(v, yp))
    gp = tp - dot(w, gq)
    left = lax.broadcasted_iota(jnp.int32, (NB, 256), 1) < NB
    here = left & (full(zl) == 0)
    is_p = here & (full(first) == full(k))
    is_q = here & (full(first) != full(k))
    zero = jnp.zeros((NB, NB), F32)
    pad_p = jnp.concatenate([pinv, zero], 1)
    pad_q = jnp.concatenate([qinv, zero], 1)
    pad_wq = jnp.concatenate([dot(w, qinv), zero], 1)
    gp = jnp.where(is_p, -pad_p, jnp.where(is_q, pad_wq, gp))
    gq = jnp.where(is_p, 0.0, jnp.where(is_q, -pad_q, gq))
    row_p = full(first) == full(x)
    row_q = (full(x) < 2) & (full(first) != full(x))
    gp0 = jnp.where(row_p, 0.0, jnp.where(row_q, jnp.where(is_p, -pad_p, tp), gp))
    gq0 = jnp.where(row_p | row_q, 0.0, gq)
    drop0 = (is_p & ~row_p) | (is_q & ~row_p & ~row_q)

    def stacked(p, q):
        return jnp.concatenate([jnp.where(wide, q, p), jnp.where(wide, p, q)], 0)

    g0, g = stacked(gp0, gq0), stacked(gp, gq)

    for j in range(1, 4):
        pl.when(plain)(across(0, j).wait_recv)
    start(sib2, plain)
    for c in cs[:-1]:
        gather(c)
    pl.when(plain)(sib2.wait_recv)
    x0 = jnp.concatenate([dx[slot, 0], dx[slot, 1]], 1)
    u[0:NB, :] = jnp.where(drop0, 0.0, f[0:NB, :]) - dot(x0, g0)
    side = {}

    def swap(c):
        for d in (1, 2, 3):
            xg[c, d].wait_recv()
        here = xf.at[k, :, c.sub]
        side[c] = copy(new(), here, here, other)
        start(side[c])

    def product(c):
        side[c].wait_recv()
        for i in range(4):
            r = NB + i * PART + c.off
            both = jnp.concatenate([xf[0, i, c.sub], xf[1, i, c.sub]], 1)
            u[r : r + c.rows, :] = dot(both, g)

    for c in bs[1:]:
        pass_on(c, far)
    swap(bs[0])
    gather(cs[-1])
    product(bs[0])
    for c in bs[1:]:
        swap(c)
    for c in bs[1:]:
        product(c)
    for c in chunks[1:]:
        for d in (1, 2, 3):
            ag[c, d].wait_recv()
        for i in range(4):
            r = slice(NB + i * PART + c.off, NB + i * PART + c.off + c.rows)
            u[r, c.cols] = f[r, c.cols] - u[r, c.cols]
    for c, cond in sends:
        if cond is None:
            c.wait_send()
        else:
            pl.when(cond)(c.wait_send)


def solution(mesh):
    rows, cols = 1024, 256

    def body(terms, order):
        vm = lambda *s: pltpu.VMEM(s, F32)
        order, terms = (
            pltpu.with_memory_space_constraint(v, pltpu.HBM)
            for v in (order, terms.reshape(rows, cols))
        )
        return pl.pallas_call(
            kernel,
            out_shape=jax.ShapeDtypeStruct((rows, cols), F32),
            in_specs=[
                pl.BlockSpec(memory_space=pltpu.HBM),
                pl.BlockSpec(memory_space=pltpu.HBM),
            ],
            out_specs=pl.BlockSpec(memory_space=pltpu.VMEM),
            scratch_shapes=[
                pltpu.SMEM((2,), jnp.int32),
                vm(rows, cols), vm(rows, cols),
                vm(3, 32, 256), vm(3, PART, 128), vm(3, PART, 128),
                vm(32, 256), vm(PART, 128), vm(PART, 128),
                vm(32, 256), vm(PART, 128), vm(PART, 128),
                vm(2, 32, 128), vm(32, 128), vm(3, 2, 128, 128), vm(2, 128, 256),
                vm(2, 4, PART, 128), vm(2, 128, 128),
                pltpu.SemaphoreType.DMA((4,)),
                pltpu.SemaphoreType.DMA((128,)),
                pltpu.SemaphoreType.DMA((128,)),
            ],
            compiler_params=pltpu.CompilerParams(collective_id=0, has_side_effects=True, vmem_limit_bytes=48 << 20),
            name="front",
        )(order, terms)

    return jax.shard_map(
        body,
        mesh=mesh,
        in_specs=(P("layer", "row", "col"), P()),
        out_specs=P("row", "col"),
        check_vma=False,
    )
```

```python
import functools

import jax
import jax.numpy as jnp
from jax import lax
from jax.experimental import pallas as pl
from jax.experimental.pallas import tpu as pltpu
from jax.sharding import PartitionSpec as P

MESH = pl.DeviceIdType.MESH
NB = 128
F32 = jnp.float32
PART = 224
SPLIT = (96, 128)


def dev(y, z, x, k):
    y, z, x = lax.rem(y + 8, 4), lax.rem(z + 32, 16), lax.rem(x + 8, 4)
    return (y * 2 + z // 8, x, lax.rem(z, 8) * 2 + k)


def dot(a, b):
    return jnp.dot(a, b, precision=lax.Precision.HIGHEST, preferred_element_type=F32)


def inverse_steps(v, lo, hi):
    n = NB
    lane8 = lax.broadcasted_iota(jnp.int32, (8, n), 1)
    sub8 = lax.broadcasted_iota(jnp.int32, (8, n), 0)
    subc = lax.broadcasted_iota(jnp.int32, (8, 8, n), 1)
    colc = lax.broadcasted_iota(jnp.int32, (8, 8, n), 0)
    lane = lax.broadcasted_iota(jnp.int32, (n, n), 1)
    for b in range(lo, hi):
        o = b * 8
        v0 = v[o : o + 8, :]
        c = jnp.stack([jnp.broadcast_to(v0[:, o + s : o + s + 1], (8, n)) for s in range(8)])
        for s in range(8):
            row = c[:, s : s + 1, :]
            pinv = 1.0 / row[s : s + 1]
            row = jnp.where(colc[:, :1] == s, pinv, row * pinv)
            base = jnp.where(colc == s, 0.0, c)
            c = jnp.where(subc == s, jnp.broadcast_to(row, (8, 8, n)), base - c[s : s + 1] * row)
        eye = (lane8 - o == sub8).astype(F32)
        v0 = jnp.where((lane8 >= o) & (lane8 < o + 8), eye, v0)
        r = c[0] * v0[0:1]
        for s in range(1, 8):
            r = r + c[s] * v0[s : s + 1]
        acc = jnp.where((lane >= o) & (lane < o + 8), 0.0, v)
        for s in range(8):
            acc = acc - v[:, o + s : o + s + 1] * r[s : s + 1]
        parts = [acc[:o]] if o else []
        parts += [r, acc[o + 8 :]] if o + 8 < n else [r]
        v = jnp.concatenate(parts, 0)
    return v


class Chunk:
    def __init__(self, base, stride, off, rows, lo, hi, recv, part, far):
        self.base, self.stride, self.off, self.rows = base, stride, off, rows
        self.cols = slice(lo, hi)
        self.sub = slice(off, off + rows)
        self.recv, self.part, self.far = recv, part, far

    def at(self, ref, y):
        start = pl.multiple_of(self.base + y * self.stride + self.off, 8)
        return ref.at[pl.ds(start, self.rows), self.cols]

    def mine(self, ref, *lead):
        return ref.at[(*lead, self.sub)]


def kernel(
    order_hbm, t_hbm, u,
    order_ref, t, f, ra, rb, rc, pa, pb, pc, za, zb, zc, xh, xa, dx, yb, xf, mat,
    in_sem, ssem, rsem,
):
    layer, x, col = lax.axis_index("layer"), lax.axis_index("row"), lax.axis_index("col")
    y, zl, k = layer // 2, col // 2, lax.rem(col, 2)
    zh = lax.rem(layer, 2)
    z = zh * 8 + zl
    source, relay = zl == 0, (zl == 2) | (zl == 6)
    other = dev(y, z, x, 1 - k)
    count = [0]
    sends = []

    def new():
        count[0] += 1
        return count[0] - 1

    def copy(i, src, dst, target, j=None):
        return pltpu.make_async_remote_copy(
            src_ref=src, dst_ref=dst, send_sem=ssem.at[i],
            recv_sem=rsem.at[i if j is None else j], device_id=target, device_id_type=MESH,
        )

    def start(c, cond=None):
        if cond is None:
            c.start()
        else:
            pl.when(cond)(c.start)
        sends.append((c, cond))

    a = Chunk(0, 32, 0, 32, 0, 256, ra, pa, za)
    bs, cs, off = [], [], 0
    for n in SPLIT:
        bs.append(Chunk(NB, PART, off, n, 0, 128, rb, pb, zb))
        cs.append(Chunk(NB, PART, off, n, 128, 256, rc, pc, zc))
        off += n
    chunks = [a, *bs, *cs]

    loads = [
        pltpu.make_async_copy(t_hbm.at[r, c], t.at[r, c], in_sem.at[i])
        for i, (r, c) in enumerate(
            [
                (slice(0, 128), slice(0, 256)),
                (slice(128, 1024), slice(0, 128)),
                (slice(128, 1024), slice(128, 256)),
            ]
        )
    ]
    loads.append(pltpu.make_async_copy(order_hbm, order_ref, in_sem.at[3]))
    for c in loads:
        c.start()

    barrier = pltpu.get_barrier_semaphore()
    peers = [dev(y + i, z, x + j, k) for i in range(4) for j in range(4) if i or j]
    peers += [dev(y, z + d, x, k) for d in range(1, 16)]
    peers += [other]
    for p in peers:
        pl.semaphore_signal(barrier, inc=1, device_id=p, device_id_type=MESH)
    pl.semaphore_wait(barrier, len(peers))

    rs, zx = {}, {}
    for n, c in enumerate(chunks):
        if n in (0, 1, 1 + len(bs)):
            loads[0 if n == 0 else 1 if n == 1 else 2].wait()
        for d in (1, 3, 2):
            y2 = lax.rem(y + d, 4)
            rs[c, d] = copy(new(), c.at(t, y2), c.mine(c.recv, d - 1), dev(y2, z, x, k))
            start(rs[c, d])

    def half_sum(c):
        for d in (1, 2, 3):
            rs[c, d].wait_recv()
        own, got = c.at(t, y), [c.mine(c.recv, d)[...] for d in range(3)]
        c.mine(c.part)[...] = (own[...] + got[0]) + (got[1] + got[2])
        zx[c] = copy(new(), c.mine(c.part), c.mine(c.far), dev(y, z + 8, x, k))
        sends.append((zx[c], None))

    def full_sum(c):
        zx[c].wait_recv()
        return c.mine(c.part)[...] + c.mine(c.far)[...]

    half_sum(a)
    xhalf = {}
    for d in (1, 15, 2, 14, 3, 13, 4, 12, 5, 11, 6, 10, 7, 9, 8):
        i = new()
        if not xhalf:
            xhalf[0], xhalf[1] = i, new()
        for h in range(2):
            c = copy(i, pa.at[:, :128], xh.at[h], dev(y, z + d, x, k), xhalf[h])
            start(c, source & (zh == h))
    panel = x < 2
    plain, inner = jnp.logical_not(panel), jnp.logical_not(source)
    leaf = jnp.logical_not(source | relay)
    far = (zl == 3) | (zl == 4) | (zl == 5)
    near = jnp.logical_not(source | far)
    pl.when(plain)(zx[a].start)
    half_sum(bs[0])
    pl.when(panel)(zx[a].start)
    pl.when(plain)(zx[bs[0]].start)
    for c in bs[1:]:
        half_sum(c)
    pl.when(panel)(zx[bs[0]].start)
    for c in bs[1:]:
        zx[c].start()
    half_sum(cs[0])
    pl.when(inner)(zx[cs[0]].start)

    slot = jnp.minimum(x, 2)
    rows_y = pl.ds(pl.multiple_of(y * 32, 8), 32)
    plane = {(i, j): new() for i in (0, 1, 3, 2) for j in (0, 1, 3, 2) if i or j}

    def across(i, j):
        return copy(plane[i, j], xa, dx.at[slot, k, rows_y], dev(y + j, z, x + i, k))

    def columns(cond):
        for h in range(2):

            @pl.when(cond & source & (zh == h))
            def _(h=h):
                xh[h] = pa[:, :128]

            @pl.when(cond & jnp.logical_not(source & (zh == h)))
            def _(h=h):
                copy(xhalf[h], xh.at[h], xh.at[h], other).wait_recv()

        @pl.when(cond)
        def _():
            xa[...] = xh[0] + xh[1]
            dx[slot, k, rows_y] = xa[...]

        for i, j in plane:
            if cond is panel or not i:
                start(across(i, j), cond)

    columns(panel)
    for c in cs[1:]:
        half_sum(c)
        pl.when(leaf)(zx[c].start)

    f[rows_y, :] = full_sum(a)
    ag = {}
    for d in (1, 3, 2):
        ag[a, d] = copy(new(), f.at[rows_y], f.at[rows_y], dev(y + d, z, x, k))
        start(ag[a, d])
    rows_of = {}
    for dxx in (1, 3, 2):
        for dy in range(4):
            rows_of[dxx, dy] = copy(
                new(), f.at[rows_y], yb.at[jnp.minimum(x, 1), rows_y],
                dev(y + dy, z, x + dxx, k),
            )
            start(rows_of[dxx, dy], panel)

    branch, xg = {}, {}

    def spread(c, cond):
        for d in (1, 3, 2):
            pl.when(cond)(xg[c, d].start)

    def gather(c):
        zx[c].wait_recv()
        total = c.mine(c.part)[...] + c.mine(c.far)[...]
        if c in bs:
            here = c.mine(xf, k, y)
            branch[c] = [new() for _ in range(4)]
            for d in (1, 3, 2):
                xg[c, d] = copy(new(), here, here, dev(y + d, z, x, k))
                sends.append((xg[c, d], None))

            @pl.when(source)
            def _():
                here[...] = total

            for i, d in zip(branch[c], (2, -2, 1, -1)):
                start(copy(i, here, here, dev(y, z + d, x, k), branch[c][0]), source)
            spread(c, source)
            total = jnp.where(jnp.full((c.rows, 128), zl, jnp.int32) == 0, 0.0, total)
        c.at(f, y)[...] = total
        for d in (1, 3, 2):
            ag[c, d] = copy(new(), c.at(f, y), c.at(f, y), dev(y + d, z, x, k))
            start(ag[c, d])

    def pass_on(c, cond):
        here = c.mine(xf, k, y)
        i, i2 = branch[c][:2]

        @pl.when(cond)
        def _():
            copy(i, here, here, other).wait_recv()

        if cond is near:
            start(copy(i, here, here, dev(y, z + 2, x, k), i), zl == 2)
            start(copy(i2, here, here, dev(y, z + 1, x, k), i), zl == 2)
            start(copy(i, here, here, dev(y, z - 1, x, k), i), zl == 6)
        spread(c, cond)

    for i, j in plane:
        pl.when(lax.rem(x - i + 4, 4) < 2)(across(i, j).wait_recv)
    sib = copy(new(), dx.at[0:2, k], dx.at[0:2, k], other)
    start(sib)
    sib2 = copy(new(), dx.at[2, k], dx.at[2, k], other)
    gather(bs[0])
    pl.when(source)(zx[cs[0]].start)
    sib.wait_recv()

    loads[3].wait()
    first = order_ref[0]
    swapped = jnp.full((NB, NB), first, jnp.int32) == 1
    d00, d01, d10, d11 = dx[0, 0], dx[0, 1], dx[1, 0], dx[1, 1]
    dpp, dqq = jnp.where(swapped, d11, d00), jnp.where(swapped, d00, d11)
    dpq, dqp = jnp.where(swapped, d10, d01), jnp.where(swapped, d01, d10)

    mat[0] = inverse_steps(dpp, 0, 8)
    pass_on(bs[0], near)
    for c in cs[1:]:
        pl.when(relay)(zx[c].start)
    for c in bs[1:]:
        gather(c)
    for c in cs[1:]:
        pl.when(source)(zx[c].start)
    mat[0] = inverse_steps(mat[0], 8, 16)
    pinv = mat[0]
    w = dot(pinv, dpq)
    v = dot(dqp, pinv)
    mat[1] = dqq - dot(dqp, w)
    mat[1] = inverse_steps(mat[1], 0, 8)
    for c in bs[1:]:
        pass_on(c, near)
    mat[1] = inverse_steps(mat[1], 8, 16)
    qinv = mat[1]
    pass_on(bs[0], far)
    columns(plain)

    for d in (1, 2, 3):
        ag[a, d].wait_recv()
    for (dxx, dy), c in rows_of.items():
        pl.when(lax.rem(x - dxx + 4, 4) < 2)(c.wait_recv)
    for i in range(2):

        @pl.when(x == i)
        def _(i=i):
            yb[i] = f[0:NB, :]

    def full(value):
        return jnp.full((NB, 256), value, jnp.int32)

    wide = full(first) == 1
    y0, y1 = yb[0], yb[1]
    yp, yq = jnp.where(wide, y1, y0), jnp.where(wide, y0, y1)
    tp = dot(pinv, yp)
    gq = dot(qinv, yq - dot(v, yp))
    gp = tp - dot(w, gq)
    left = lax.broadcasted_iota(jnp.int32, (NB, 256), 1) < NB
    here = left & (full(zl) == 0)
    is_p = here & (full(first) == full(k))
    is_q = here & (full(first) != full(k))
    zero = jnp.zeros((NB, NB), F32)
    pad_p = jnp.concatenate([pinv, zero], 1)
    pad_q = jnp.concatenate([qinv, zero], 1)
    pad_wq = jnp.concatenate([dot(w, qinv), zero], 1)
    gp = jnp.where(is_p, -pad_p, jnp.where(is_q, pad_wq, gp))
    gq = jnp.where(is_p, 0.0, jnp.where(is_q, -pad_q, gq))
    row_p = full(first) == full(x)
    row_q = (full(x) < 2) & (full(first) != full(x))
    gp0 = jnp.where(row_p, 0.0, jnp.where(row_q, jnp.where(is_p, -pad_p, tp), gp))
    gq0 = jnp.where(row_p | row_q, 0.0, gq)
    drop0 = (is_p & ~row_p) | (is_q & ~row_p & ~row_q)

    def stacked(p, q):
        return jnp.concatenate([jnp.where(wide, q, p), jnp.where(wide, p, q)], 0)

    g0, g = stacked(gp0, gq0), stacked(gp, gq)

    for j in range(1, 4):
        pl.when(plain)(across(0, j).wait_recv)
    start(sib2, plain)
    for c in cs[:-1]:
        gather(c)
    pl.when(plain)(sib2.wait_recv)
    x0 = jnp.concatenate([dx[slot, 0], dx[slot, 1]], 1)
    u[0:NB, :] = jnp.where(drop0, 0.0, f[0:NB, :]) - dot(x0, g0)
    side = {}

    def swap(c):
        for d in (1, 2, 3):
            xg[c, d].wait_recv()
        here = xf.at[k, :, c.sub]
        side[c] = copy(new(), here, here, other)
        start(side[c])

    def product(c):
        side[c].wait_recv()
        for i in range(4):
            r = NB + i * PART + c.off
            both = jnp.concatenate([xf[0, i, c.sub], xf[1, i, c.sub]], 1)
            u[r : r + c.rows, :] = dot(both, g)

    for c in bs[1:]:
        pass_on(c, far)
    swap(bs[0])
    gather(cs[-1])
    product(bs[0])
    for c in bs[1:]:
        swap(c)
    for c in bs[1:]:
        product(c)
    for c in chunks[1:]:
        for d in (1, 2, 3):
            ag[c, d].wait_recv()
        for i in range(4):
            r = slice(NB + i * PART + c.off, NB + i * PART + c.off + c.rows)
            u[r, c.cols] = f[r, c.cols] - u[r, c.cols]
    for c, cond in sends:
        if cond is None:
            c.wait_send()
        else:
            pl.when(cond)(c.wait_send)


def solution(mesh):
    rows, cols = 1024, 256

    def body(terms, order):
        vm = lambda *s: pltpu.VMEM(s, F32)
        order, terms = (
            pltpu.with_memory_space_constraint(v, pltpu.HBM)
            for v in (order, terms.reshape(rows, cols))
        )
        return pl.pallas_call(
            kernel,
            out_shape=jax.ShapeDtypeStruct((rows, cols), F32),
            in_specs=[
                pl.BlockSpec(memory_space=pltpu.HBM),
                pl.BlockSpec(memory_space=pltpu.HBM),
            ],
            out_specs=pl.BlockSpec(memory_space=pltpu.VMEM),
            scratch_shapes=[
                pltpu.SMEM((2,), jnp.int32),
                vm(rows, cols), vm(rows, cols),
                vm(3, 32, 256), vm(3, PART, 128), vm(3, PART, 128),
                vm(32, 256), vm(PART, 128), vm(PART, 128),
                vm(32, 256), vm(PART, 128), vm(PART, 128),
                vm(2, 32, 128), vm(32, 128), vm(3, 2, 128, 128), vm(2, 128, 256),
                vm(2, 4, PART, 128), vm(2, 128, 128),
                pltpu.SemaphoreType.DMA((4,)),
                pltpu.SemaphoreType.DMA((128,)),
                pltpu.SemaphoreType.DMA((128,)),
            ],
            compiler_params=pltpu.CompilerParams(collective_id=0, has_side_effects=True, vmem_limit_bytes=48 << 20),
            name="front",
        )(order, terms)

    return jax.shard_map(
        body,
        mesh=mesh,
        in_specs=(P("layer", "row", "col"), P()),
        out_specs=P("row", "col"),
        check_vma=False,
    )
```

```python
import functools

import jax
import jax.numpy as jnp
from jax import lax
from jax.experimental import pallas as pl
from jax.experimental.pallas import tpu as pltpu
from jax.sharding import PartitionSpec as P

MESH = pl.DeviceIdType.MESH
NB = 128
F32 = jnp.float32
PART = 224
SPLIT = (88, 136)


def dev(y, z, x, k):
    y, z, x = lax.rem(y + 8, 4), lax.rem(z + 32, 16), lax.rem(x + 8, 4)
    return (y * 2 + z // 8, x, lax.rem(z, 8) * 2 + k)


def dot(a, b):
    return jnp.dot(a, b, precision=lax.Precision.HIGHEST, preferred_element_type=F32)


def inverse_steps(v, lo, hi):
    n = NB
    lane8 = lax.broadcasted_iota(jnp.int32, (8, n), 1)
    sub8 = lax.broadcasted_iota(jnp.int32, (8, n), 0)
    subc = lax.broadcasted_iota(jnp.int32, (8, 8, n), 1)
    colc = lax.broadcasted_iota(jnp.int32, (8, 8, n), 0)
    lane = lax.broadcasted_iota(jnp.int32, (n, n), 1)
    for b in range(lo, hi):
        o = b * 8
        v0 = v[o : o + 8, :]
        c = jnp.stack([jnp.broadcast_to(v0[:, o + s : o + s + 1], (8, n)) for s in range(8)])
        for s in range(8):
            row = c[:, s : s + 1, :]
            pinv = 1.0 / row[s : s + 1]
            row = jnp.where(colc[:, :1] == s, pinv, row * pinv)
            base = jnp.where(colc == s, 0.0, c)
            c = jnp.where(subc == s, jnp.broadcast_to(row, (8, 8, n)), base - c[s : s + 1] * row)
        eye = (lane8 - o == sub8).astype(F32)
        v0 = jnp.where((lane8 >= o) & (lane8 < o + 8), eye, v0)
        r = c[0] * v0[0:1]
        for s in range(1, 8):
            r = r + c[s] * v0[s : s + 1]
        acc = jnp.where((lane >= o) & (lane < o + 8), 0.0, v)
        for s in range(8):
            acc = acc - v[:, o + s : o + s + 1] * r[s : s + 1]
        parts = [acc[:o]] if o else []
        parts += [r, acc[o + 8 :]] if o + 8 < n else [r]
        v = jnp.concatenate(parts, 0)
    return v


class Chunk:
    def __init__(self, base, stride, off, rows, lo, hi, recv, part, far):
        self.base, self.stride, self.off, self.rows = base, stride, off, rows
        self.cols = slice(lo, hi)
        self.sub = slice(off, off + rows)
        self.recv, self.part, self.far = recv, part, far

    def at(self, ref, y):
        start = pl.multiple_of(self.base + y * self.stride + self.off, 8)
        return ref.at[pl.ds(start, self.rows), self.cols]

    def mine(self, ref, *lead):
        return ref.at[(*lead, self.sub)]


def kernel(
    order_hbm, t_hbm, u,
    order_ref, t, f, ra, rb, rc, pa, pb, pc, za, zb, zc, xh, xa, dx, yb, xf, mat,
    in_sem, ssem, rsem,
):
    layer, x, col = lax.axis_index("layer"), lax.axis_index("row"), lax.axis_index("col")
    y, zl, k = layer // 2, col // 2, lax.rem(col, 2)
    zh = lax.rem(layer, 2)
    z = zh * 8 + zl
    source, relay = zl == 0, (zl == 2) | (zl == 6)
    other = dev(y, z, x, 1 - k)
    count = [0]
    sends = []

    def new():
        count[0] += 1
        return count[0] - 1

    def copy(i, src, dst, target, j=None):
        return pltpu.make_async_remote_copy(
            src_ref=src, dst_ref=dst, send_sem=ssem.at[i],
            recv_sem=rsem.at[i if j is None else j], device_id=target, device_id_type=MESH,
        )

    def start(c, cond=None):
        if cond is None:
            c.start()
        else:
            pl.when(cond)(c.start)
        sends.append((c, cond))

    a = Chunk(0, 32, 0, 32, 0, 256, ra, pa, za)
    bs, cs, off = [], [], 0
    for n in SPLIT:
        bs.append(Chunk(NB, PART, off, n, 0, 128, rb, pb, zb))
        cs.append(Chunk(NB, PART, off, n, 128, 256, rc, pc, zc))
        off += n
    chunks = [a, *bs, *cs]

    loads = [
        pltpu.make_async_copy(t_hbm.at[r, c], t.at[r, c], in_sem.at[i])
        for i, (r, c) in enumerate(
            [
                (slice(0, 128), slice(0, 256)),
                (slice(128, 1024), slice(0, 128)),
                (slice(128, 1024), slice(128, 256)),
            ]
        )
    ]
    loads.append(pltpu.make_async_copy(order_hbm, order_ref, in_sem.at[3]))
    for c in loads:
        c.start()

    barrier = pltpu.get_barrier_semaphore()
    peers = [dev(y + i, z, x + j, k) for i in range(4) for j in range(4) if i or j]
    peers += [dev(y, z + d, x, k) for d in range(1, 16)]
    peers += [other]
    for p in peers:
        pl.semaphore_signal(barrier, inc=1, device_id=p, device_id_type=MESH)
    pl.semaphore_wait(barrier, len(peers))

    rs, zx = {}, {}
    for n, c in enumerate(chunks):
        if n in (0, 1, 1 + len(bs)):
            loads[0 if n == 0 else 1 if n == 1 else 2].wait()
        for d in (1, 3, 2):
            y2 = lax.rem(y + d, 4)
            rs[c, d] = copy(new(), c.at(t, y2), c.mine(c.recv, d - 1), dev(y2, z, x, k))
            start(rs[c, d])

    def half_sum(c):
        for d in (1, 2, 3):
            rs[c, d].wait_recv()
        own, got = c.at(t, y), [c.mine(c.recv, d)[...] for d in range(3)]
        c.mine(c.part)[...] = (own[...] + got[0]) + (got[1] + got[2])
        zx[c] = copy(new(), c.mine(c.part), c.mine(c.far), dev(y, z + 8, x, k))
        sends.append((zx[c], None))

    def full_sum(c):
        zx[c].wait_recv()
        return c.mine(c.part)[...] + c.mine(c.far)[...]

    half_sum(a)
    xhalf = {}
    for d in (1, 15, 2, 14, 3, 13, 4, 12, 5, 11, 6, 10, 7, 9, 8):
        i = new()
        if not xhalf:
            xhalf[0], xhalf[1] = i, new()
        for h in range(2):
            c = copy(i, pa.at[:, :128], xh.at[h], dev(y, z + d, x, k), xhalf[h])
            start(c, source & (zh == h))
    panel = x < 2
    plain, inner = jnp.logical_not(panel), jnp.logical_not(source)
    leaf = jnp.logical_not(source | relay)
    far = (zl == 3) | (zl == 4) | (zl == 5)
    near = jnp.logical_not(source | far)
    pl.when(plain)(zx[a].start)
    half_sum(bs[0])
    pl.when(panel)(zx[a].start)
    pl.when(plain)(zx[bs[0]].start)
    for c in bs[1:]:
        half_sum(c)
    pl.when(panel)(zx[bs[0]].start)
    for c in bs[1:]:
        zx[c].start()
    half_sum(cs[0])
    pl.when(inner)(zx[cs[0]].start)

    slot = jnp.minimum(x, 2)
    rows_y = pl.ds(pl.multiple_of(y * 32, 8), 32)
    plane = {(i, j): new() for i in (0, 1, 3, 2) for j in (0, 1, 3, 2) if i or j}

    def across(i, j):
        return copy(plane[i, j], xa, dx.at[slot, k, rows_y], dev(y + j, z, x + i, k))

    def columns(cond):
        for h in range(2):

            @pl.when(cond & source & (zh == h))
            def _(h=h):
                xh[h] = pa[:, :128]

            @pl.when(cond & jnp.logical_not(source & (zh == h)))
            def _(h=h):
                copy(xhalf[h], xh.at[h], xh.at[h], other).wait_recv()

        @pl.when(cond)
        def _():
            xa[...] = xh[0] + xh[1]
            dx[slot, k, rows_y] = xa[...]

        for i, j in plane:
            if cond is panel or not i:
                start(across(i, j), cond)

    columns(panel)
    for c in cs[1:]:
        half_sum(c)
        pl.when(leaf)(zx[c].start)

    f[rows_y, :] = full_sum(a)
    ag = {}
    for d in (1, 3, 2):
        ag[a, d] = copy(new(), f.at[rows_y], f.at[rows_y], dev(y + d, z, x, k))
        start(ag[a, d])
    rows_of = {}
    for dxx in (1, 3, 2):
        for dy in range(4):
            rows_of[dxx, dy] = copy(
                new(), f.at[rows_y], yb.at[jnp.minimum(x, 1), rows_y],
                dev(y + dy, z, x + dxx, k),
            )
            start(rows_of[dxx, dy], panel)

    branch, xg = {}, {}

    def spread(c, cond):
        for d in (1, 3, 2):
            pl.when(cond)(xg[c, d].start)

    def gather(c):
        zx[c].wait_recv()
        total = c.mine(c.part)[...] + c.mine(c.far)[...]
        if c in bs:
            here = c.mine(xf, k, y)
            branch[c] = [new() for _ in range(4)]
            for d in (1, 3, 2):
                xg[c, d] = copy(new(), here, here, dev(y + d, z, x, k))
                sends.append((xg[c, d], None))

            @pl.when(source)
            def _():
                here[...] = total

            for i, d in zip(branch[c], (2, -2, 1, -1)):
                start(copy(i, here, here, dev(y, z + d, x, k), branch[c][0]), source)
            spread(c, source)
            total = jnp.where(jnp.full((c.rows, 128), zl, jnp.int32) == 0, 0.0, total)
        c.at(f, y)[...] = total
        for d in (1, 3, 2):
            ag[c, d] = copy(new(), c.at(f, y), c.at(f, y), dev(y + d, z, x, k))
            start(ag[c, d])

    def pass_on(c, cond):
        here = c.mine(xf, k, y)
        i, i2 = branch[c][:2]

        @pl.when(cond)
        def _():
            copy(i, here, here, other).wait_recv()

        if cond is near:
            start(copy(i, here, here, dev(y, z + 2, x, k), i), zl == 2)
            start(copy(i2, here, here, dev(y, z + 1, x, k), i), zl == 2)
            start(copy(i, here, here, dev(y, z - 1, x, k), i), zl == 6)
        spread(c, cond)

    for i, j in plane:
        pl.when(lax.rem(x - i + 4, 4) < 2)(across(i, j).wait_recv)
    sib = copy(new(), dx.at[0:2, k], dx.at[0:2, k], other)
    start(sib)
    sib2 = copy(new(), dx.at[2, k], dx.at[2, k], other)
    gather(bs[0])
    pl.when(source)(zx[cs[0]].start)
    sib.wait_recv()

    loads[3].wait()
    first = order_ref[0]
    swapped = jnp.full((NB, NB), first, jnp.int32) == 1
    d00, d01, d10, d11 = dx[0, 0], dx[0, 1], dx[1, 0], dx[1, 1]
    dpp, dqq = jnp.where(swapped, d11, d00), jnp.where(swapped, d00, d11)
    dpq, dqp = jnp.where(swapped, d10, d01), jnp.where(swapped, d01, d10)

    mat[0] = inverse_steps(dpp, 0, 8)
    pass_on(bs[0], near)
    for c in cs[1:]:
        pl.when(relay)(zx[c].start)
    for c in bs[1:]:
        gather(c)
    for c in cs[1:]:
        pl.when(source)(zx[c].start)
    mat[0] = inverse_steps(mat[0], 8, 16)
    pinv = mat[0]
    w = dot(pinv, dpq)
    v = dot(dqp, pinv)
    mat[1] = dqq - dot(dqp, w)
    mat[1] = inverse_steps(mat[1], 0, 8)
    for c in bs[1:]:
        pass_on(c, near)
    mat[1] = inverse_steps(mat[1], 8, 16)
    qinv = mat[1]
    pass_on(bs[0], far)
    columns(plain)

    for d in (1, 2, 3):
        ag[a, d].wait_recv()
    for (dxx, dy), c in rows_of.items():
        pl.when(lax.rem(x - dxx + 4, 4) < 2)(c.wait_recv)
    for i in range(2):

        @pl.when(x == i)
        def _(i=i):
            yb[i] = f[0:NB, :]

    def full(value):
        return jnp.full((NB, 256), value, jnp.int32)

    wide = full(first) == 1
    y0, y1 = yb[0], yb[1]
    yp, yq = jnp.where(wide, y1, y0), jnp.where(wide, y0, y1)
    tp = dot(pinv, yp)
    gq = dot(qinv, yq - dot(v, yp))
    gp = tp - dot(w, gq)
    left = lax.broadcasted_iota(jnp.int32, (NB, 256), 1) < NB
    here = left & (full(zl) == 0)
    is_p = here & (full(first) == full(k))
    is_q = here & (full(first) != full(k))
    zero = jnp.zeros((NB, NB), F32)
    pad_p = jnp.concatenate([pinv, zero], 1)
    pad_q = jnp.concatenate([qinv, zero], 1)
    pad_wq = jnp.concatenate([dot(w, qinv), zero], 1)
    gp = jnp.where(is_p, -pad_p, jnp.where(is_q, pad_wq, gp))
    gq = jnp.where(is_p, 0.0, jnp.where(is_q, -pad_q, gq))
    row_p = full(first) == full(x)
    row_q = (full(x) < 2) & (full(first) != full(x))
    gp0 = jnp.where(row_p, 0.0, jnp.where(row_q, jnp.where(is_p, -pad_p, tp), gp))
    gq0 = jnp.where(row_p | row_q, 0.0, gq)
    drop0 = (is_p & ~row_p) | (is_q & ~row_p & ~row_q)

    def stacked(p, q):
        return jnp.concatenate([jnp.where(wide, q, p), jnp.where(wide, p, q)], 0)

    g0, g = stacked(gp0, gq0), stacked(gp, gq)

    for j in range(1, 4):
        pl.when(plain)(across(0, j).wait_recv)
    start(sib2, plain)
    for c in cs[:-1]:
        gather(c)
    pl.when(plain)(sib2.wait_recv)
    x0 = jnp.concatenate([dx[slot, 0], dx[slot, 1]], 1)
    u[0:NB, :] = jnp.where(drop0, 0.0, f[0:NB, :]) - dot(x0, g0)
    side = {}

    def swap(c):
        for d in (1, 2, 3):
            xg[c, d].wait_recv()
        here = xf.at[k, :, c.sub]
        side[c] = copy(new(), here, here, other)
        start(side[c])

    def product(c):
        side[c].wait_recv()
        for i in range(4):
            r = NB + i * PART + c.off
            both = jnp.concatenate([xf[0, i, c.sub], xf[1, i, c.sub]], 1)
            u[r : r + c.rows, :] = dot(both, g)

    for c in bs[1:]:
        pass_on(c, far)
    swap(bs[0])
    gather(cs[-1])
    product(bs[0])
    for c in bs[1:]:
        swap(c)
    for c in bs[1:]:
        product(c)
    for c in chunks[1:]:
        for d in (1, 2, 3):
            ag[c, d].wait_recv()
        for i in range(4):
            r = slice(NB + i * PART + c.off, NB + i * PART + c.off + c.rows)
            u[r, c.cols] = f[r, c.cols] - u[r, c.cols]
    for c, cond in sends:
        if cond is None:
            c.wait_send()
        else:
            pl.when(cond)(c.wait_send)


def solution(mesh):
    rows, cols = 1024, 256

    def body(terms, order):
        vm = lambda *s: pltpu.VMEM(s, F32)
        order, terms = (
            pltpu.with_memory_space_constraint(v, pltpu.HBM)
            for v in (order, terms.reshape(rows, cols))
        )
        return pl.pallas_call(
            kernel,
            out_shape=jax.ShapeDtypeStruct((rows, cols), F32),
            in_specs=[
                pl.BlockSpec(memory_space=pltpu.HBM),
                pl.BlockSpec(memory_space=pltpu.HBM),
            ],
            out_specs=pl.BlockSpec(memory_space=pltpu.VMEM),
            scratch_shapes=[
                pltpu.SMEM((2,), jnp.int32),
                vm(rows, cols), vm(rows, cols),
                vm(3, 32, 256), vm(3, PART, 128), vm(3, PART, 128),
                vm(32, 256), vm(PART, 128), vm(PART, 128),
                vm(32, 256), vm(PART, 128), vm(PART, 128),
                vm(2, 32, 128), vm(32, 128), vm(3, 2, 128, 128), vm(2, 128, 256),
                vm(2, 4, PART, 128), vm(2, 128, 128),
                pltpu.SemaphoreType.DMA((4,)),
                pltpu.SemaphoreType.DMA((128,)),
                pltpu.SemaphoreType.DMA((128,)),
            ],
            compiler_params=pltpu.CompilerParams(collective_id=0, has_side_effects=True, vmem_limit_bytes=48 << 20),
            name="front",
        )(order, terms)

    return jax.shard_map(
        body,
        mesh=mesh,
        in_specs=(P("layer", "row", "col"), P()),
        out_specs=P("row", "col"),
        check_vma=False,
    )
```
